256 devices in a mesh: row: 32 (over z_lo, y, core), col: 8 (over x, z_hi).
Axes of the slice: x: 4, y: 4, z: 8 (z_hi: 2, z_lo: 4; z = z_hi * 4 + z_lo), core: 2. Of those that a mesh axis runs over, the one named last changes fastest.
Arguments:
- diag_tile: float32 [1024, 1024], P(('row', 'col')), as said below
- left_row: bfloat16 [1024, 64, 256], P('col', 'row'), may hold values from -0.3984375 to 0.3984375
- right_row: bfloat16 [1024, 64, 256], P('col', 'row'), may hold values from -1.09375 to 1.09375
- right_col: bfloat16 [1024, 32, 256], P('row', 'col'), may hold values from -1.09375 to 1.09375
- bucket_row: int32 [64], P('row'), may hold values from 1 to 4
- bucket_col: int32 [32], P('col'), may hold values from 1 to 4
Outputs:
- panel_row: bfloat16 [1024, 64, 256], P('col', 'row')
- panel_col: bfloat16 [1024, 32, 256], P('row', 'col')
- update_left: bfloat16 [64, 32, 1024, 256], P('row', 'col')
The draws below stay inside these ranges and needn't reach their ends.
Inputs may be any that keep to these rules, and one draw needn't show every extreme that they name: diag_tile is symmetric positive definite. `bucket_row`: a tile's rank is 64 times its bucket; factor columns from the rank on are not part of the tile. `bucket_col`: as for bucket_row.
All inputs are finite; a program needn't handle non-finite values.
Results may differ from the reference program's by a relative error of at most 0.0062.
Values may be sent and summed in bfloat16 or wider, within the bound.
No kernel may reach another device: no remote copies, remote signals or barrier semaphores. Data moves between devices by JAX's collectives and lax.ppermute only.
A program may use at most 128 MiB of HBM per device.

```python
import jax
import jax.numpy as jnp
from jax import lax

NB = 1024
RMAX = 256
RSTEP = 64
MT = 64
NC = 32


def draw_diag_tile(key, part):
    first = jax.random.fold_in(jax.random.fold_in(key, 11), 0)
    factor = jax.random.normal(first, (NB, NB), jnp.float32) / jnp.sqrt(jnp.float32(NB))
    gram = jnp.dot(factor, factor.T, precision=lax.Precision.HIGHEST) + jnp.eye(NB, dtype=jnp.float32)
    return 0.5 * (gram + gram.T)


def with_ends(drawn, key, least, high):
    spot = [jax.random.randint(jax.random.fold_in(key, axis), (), 0, length) for axis, length in enumerate(drawn.shape)]
    main_axis = drawn.shape.index(max(drawn.shape))
    next_to = spot[:main_axis] + [(spot[main_axis] + 1) % drawn.shape[main_axis]] + spot[main_axis + 1:]
    return drawn.at[tuple(spot)].set(least).at[tuple(next_to)].set(high)


def level_of(rng, extent, cuts, smallest, high):
    factor_of = 1.0
    for axis_at, parts in cuts:
        draws = jax.random.uniform(jax.random.fold_in(jax.random.fold_in(rng, 6), axis_at), (parts,), jnp.float32, smallest / len(cuts), high / len(cuts))
        factor_of = factor_of * jnp.repeat(jnp.exp(draws), extent[axis_at] // parts).reshape((-1,) + (1,) * (len(extent) - 1 - axis_at))
    return factor_of


def normal_values(stream_key, extent, scale, limit, shards=(), kind=jnp.bfloat16):
    factor_of = level_of(stream_key, extent, shards, -0.22, 0.18) if shards else 1.0
    result = jax.random.normal(stream_key, extent, jnp.float32) * scale * factor_of
    return jnp.minimum(jnp.maximum(result, -limit), limit).astype(kind)


def setup_inputs(seed: int = 0) -> dict:
    splits = jax.random.split(jax.random.key(seed), 7)
    diag_tile = draw_diag_tile(jax.random.fold_in(splits[6], 71), 0)
    left_row = normal_values(splits[1], (NB, MT, RMAX), 0.0625, 0.3984375, ((0, 8), (1, 32)))
    right_row = normal_values(splits[2], (NB, MT, RMAX), 0.18, 1.09375, ((0, 8), (1, 32)))
    right_col = normal_values(splits[3], (NB, NC, RMAX), 0.18, 1.09375, ((0, 32), (1, 8)))
    bucket_row = with_ends(jax.random.randint(splits[4], (MT,), 1, 5), jax.random.fold_in(splits[4], 1), 1, 4).astype(jnp.int32)
    bucket_col = with_ends(jax.random.randint(splits[5], (NC,), 1, 5), jax.random.fold_in(splits[5], 1), 1, 4).astype(jnp.int32)
    return dict(diag_tile=diag_tile, left_row=left_row, right_row=right_row, right_col=right_col, bucket_row=bucket_row, bucket_col=bucket_col)


def solve_panel(inverse, right, bucket):
    live = jnp.arange(RMAX, dtype=jnp.int32)[None, :] < (RSTEP * bucket)[:, None]
    masked = jnp.where(live[None, :, :], right, jnp.zeros_like(right))
    flat = masked.astype(jnp.float32).reshape(NB, -1)
    solved = jnp.dot(inverse.astype(jnp.float32), flat.astype(jnp.float32), precision=lax.Precision.HIGHEST, preferred_element_type=jnp.float32)
    return solved.reshape(NB, bucket.shape[0], RMAX).astype(jnp.bfloat16)

def reference(diag_tile, left_row, right_row, right_col, bucket_row, bucket_col):
    lower_factor = jnp.linalg.cholesky(diag_tile)
    identity = jnp.eye(NB, dtype=jnp.float32)
    inverse = lax.linalg.triangular_solve(lower_factor, identity, left_side=True, lower=True)
    panel_row = solve_panel(inverse, right_row, bucket_row)
    panel_col = solve_panel(inverse, right_col, bucket_col)
    col_wide = panel_col.astype(jnp.float32)

    def one_tile(operands):
        basis, factor = operands
        coupling = jnp.einsum('ka,kjb->jab', factor.astype(jnp.float32), col_wide, precision=lax.Precision.HIGHEST).astype(jnp.bfloat16)
        update = jnp.einsum('ka,jab->jkb', basis.astype(jnp.float32), coupling.astype(jnp.float32), precision=lax.Precision.HIGHEST)
        return (-update).astype(jnp.bfloat16)
    update_left = lax.map(one_tile, (jnp.moveaxis(left_row, 1, 0), jnp.moveaxis(panel_row, 1, 0)))
    return (panel_row, panel_col, update_left)
```

```python
import functools

import jax
import jax.numpy as jnp
from jax import lax
from jax.experimental import pallas as pl
from jax.experimental.pallas import tpu as pltpu
from jax.sharding import Mesh
from jax.sharding import PartitionSpec as P

RSTEP = 64
F32 = jnp.float32
BF16 = jnp.bfloat16
AXES = ("zl", "y", "c", "x", "zh")
ROW = ("zl", "y", "c")
COL = ("x", "zh")
SENT = 5


def split3(x):
    high = x.astype(BF16)
    rest = x - high.astype(F32)
    middle = rest.astype(BF16)
    low = (rest - middle.astype(F32)).astype(BF16)
    return high, middle, low


def lane_copy(x, lane):
    return jnp.broadcast_to(x[:, lane : lane + 1], (8, 128))


def row_copy(x, row):
    return jnp.broadcast_to(x[row : row + 1, :], (8, 128))


def factor(groups):
    lane = lax.broadcasted_iota(jnp.int32, (8, 128), 1)
    sub = lax.broadcasted_iota(jnp.int32, (8, 128), 0)
    groups = list(groups)
    for j in range(16):
        own = [lane_copy(groups[j], 8 * j + c) for c in range(8)]
        below = {g: [lane_copy(groups[g], 8 * j + c) for c in range(8)] for g in range(j + 1, 16)}
        here = (lane >= 8 * j) & (lane < 8 * j + 8)
        x = jnp.where(here, jnp.where(lane - 8 * j == sub, 1.0, 0.0), groups[j])
        scales, rows, across = [], [], []
        for c in range(8):
            scale = lax.rsqrt(row_copy(own[c], c))
            column = own[c] * scale
            row = row_copy(x, c) * scale
            x = jnp.where(sub == c, row, x) - jnp.where(sub > c, column, 0.0) * row
            lower = {d: row_copy(column, d) for d in range(c + 1, 8)}
            for d in range(c + 1, 8):
                own[d] = own[d] - column * lower[d]
            scales.append(scale)
            rows.append(row)
            across.append(lower)
        groups[j] = x
        for g in range(j + 1, 16):
            cols = below[g]
            w = jnp.where(here, 0.0, groups[g])
            for c in range(8):
                column = cols[c] * scales[c]
                for d in range(c + 1, 8):
                    cols[d] = cols[d] - column * across[c][d]
                w = w - column * rows[c]
            groups[g] = w
    return groups


def dot6(left, right, dims=((1,), (0,))):
    (lh, lm, ll), (rh, rm, rl) = left, right
    dot = functools.partial(lax.dot_general, dimension_numbers=(dims, ((), ())), preferred_element_type=F32)
    lk, rk = dims[0][0], dims[1][0]
    join = lambda a, b, d: jnp.concatenate([a, b], axis=d)
    return (
        dot(join(lh, lm, lk), join(rh, rm, rk))
        + dot(join(lh, lm, lk), join(rm, rh, rk))
        + dot(join(lh, ll, lk), join(rl, rh, rk))
    )


def long_dot6(left, right):
    (lh, lm, ll), (rh, rm, rl) = left, right
    dot = functools.partial(jnp.dot, preferred_element_type=F32)
    return dot(lh, rh) + (dot(lm, rh) + dot(lh, rm)) + (dot(lm, rm) + (dot(ll, rh) + dot(lh, rl)))


def chol_kernel(
    core_ref, mine_ref, other_ref, high_ref, mid_ref, row_ref, low_ref, lh_ref, lm_ref, ll_ref, diag_ref, dh_ref, dm_ref, dl_ref, a_ref
):
    lane = lax.broadcasted_iota(jnp.int32, (128, 128), 1)
    sub = lax.broadcasted_iota(jnp.int32, (128, 128), 0)
    col = lax.broadcasted_iota(jnp.int32, (128, 1024), 1)
    xs_refs = (high_ref, mid_ref, low_ref)
    ls_refs = (lh_ref, lm_ref, ll_ref)
    ds_refs = (dh_ref, dm_ref, dl_ref)
    for ref in (*xs_refs, *ls_refs, *ds_refs, row_ref):
        ref[...] = jnp.zeros_like(ref)
    core = core_ref[0]
    for y in range(4):
        for x in range(4):
            for z in range(4):
                group = z * 2 + y // 2
                for part_ref, half in ((mine_ref, core), (other_ref, 1 - core)):
                    rows = pl.ds(pl.multiple_of(z * 256 + y * 64 + x * 8 + half * 32, 8), 8)
                    for m in range(SENT):
                        block = (group + m) % 8
                        if m == 4 and block < group:
                            continue
                        lanes = slice(128 * m, 128 * m + 128)
                        pieces = [part_ref[4 * y + x, 2 * z + end, :, lanes] for end in range(2)]
                        a_ref[rows, 128 * block : 128 * block + 128] = jnp.concatenate(pieces, axis=0)
    for group in range(5, 8):
        for block in range(group - 4):
            a_ref[128 * block : 128 * block + 128, 128 * group : 128 * group + 128] = jnp.transpose(
                a_ref[128 * group : 128 * group + 128, 128 * block : 128 * block + 128], (1, 0)
            )
    diag_ref[...] = a_ref[0:128, 0:128]

    def settle(at):
        for ref in xs_refs:
            ref[:, pl.ds(at, 128)] = jnp.zeros((1024, 128), BF16)
        row_ref[:, pl.ds(at, 128)] = jnp.where(lane == sub, 1.0, 0.0)
        x = dot6(tuple(ref[...] for ref in ds_refs), split3(row_ref[...]))
        for ref, part in zip(xs_refs, split3(x)):
            ref[pl.ds(at, 128), :] = part
        return x

    def step(k, _):
        at = pl.multiple_of(k * 128, 128)
        before = pl.multiple_of(lax.rem(k + 7, 8) * 128, 128)
        after = pl.multiple_of(lax.rem(k + 1, 8) * 128, 128)
        groups = factor([diag_ref[8 * g : 8 * g + 8, :] for g in range(16)])
        inv = split3(jnp.where(lane <= sub, jnp.concatenate(groups, axis=0), 0.0))
        x = settle(before)
        for ref, part in zip(ls_refs, split3(jnp.transpose(x, (1, 0)))):
            ref[:, pl.ds(before, 128)] = part
        upd = long_dot6(
            tuple(ref[pl.ds(at, 128), :] for ref in ls_refs), tuple(ref[...] for ref in xs_refs)
        )
        row_ref[...] = jnp.where(col >= at, a_ref[pl.ds(at, 128), :], 0.0) - upd
        ahead = a_ref[pl.ds(after, 128), pl.ds(after, 128)] - long_dot6(
            tuple(ref[pl.ds(after, 128), :] for ref in ls_refs),
            tuple(ref[:, pl.ds(after, 128)] for ref in xs_refs),
        )
        side = row_ref[:, pl.ds(after, 128)]
        side_t = split3(jnp.transpose(side, (1, 0)))
        for ref, part in zip(ds_refs, inv):
            ref[...] = part
        x = dot6(inv, split3(side))
        xt = dot6(side_t, inv, ((1,), (1,)))
        diag_ref[...] = ahead - dot6(split3(xt), split3(x))
        return 0

    lax.fori_loop(0, 8, step, 0)
    settle(896)


def chol_inverse(core, mine, other):
    n = 1024
    whole = pl.BlockSpec(memory_space=pltpu.VMEM)
    return pl.pallas_call(
        chol_kernel,
        out_shape=[jax.ShapeDtypeStruct((n, n), BF16)] * 2,
        in_specs=[pl.BlockSpec(memory_space=pltpu.SMEM), whole, whole],
        out_specs=[whole] * 2,
        scratch_shapes=[
            pltpu.VMEM((128, n), F32),
            *[pltpu.VMEM((n, n), BF16)] * 4,
            pltpu.VMEM((128, 128), F32),
            *[pltpu.VMEM((128, 128), BF16)] * 3,
            pltpu.VMEM((n, n), F32),
        ],
        compiler_params=pltpu.CompilerParams(vmem_limit_bytes=40 * 1024 * 1024),
        cost_estimate=pl.CostEstimate(flops=20 * 10**9, bytes_accessed=8 * 2**20, transcendentals=0),
        name="chol_inverse",
    )(core, mine, other)


def panel_kernel(place_ref, row_ref, col_ref, high_ref, mid_ref, near_ref, far_ref, pr_ref, pc_ref, out_ref, p_ref):
    lane = lax.broadcasted_iota(jnp.int32, (256, 256), 1)
    step = pl.program_id(0)

    @pl.when(step == 0)
    def _():
        for i in range(4):
            depth = 256 * (i + 1)
            rows = slice(256 * i, depth)
            high, mid = high_ref[rows, :depth], mid_ref[rows, :depth]
            for t in range(6):
                if t < 2:
                    right = near_ref[: depth // 128, 0, t].reshape(depth, 256)
                    live = RSTEP * row_ref[t]
                else:
                    right = far_ref[: depth // 32, t - 2].reshape(depth, 256)
                    live = RSTEP * col_ref[t - 2]
                solved = jnp.dot(high, right, preferred_element_type=F32)
                solved = solved + jnp.dot(mid, right, preferred_element_type=F32)
                p_ref[t, rows, :] = jnp.where(lane < live, solved, 0.0).astype(BF16)
        for t in range(2):
            pr_ref[t] = p_ref[t, pl.ds(pl.multiple_of(place_ref[0] * 128, 128), 128), :]
        for t in range(4):
            pc_ref[t] = p_ref[2 + t, pl.ds(pl.multiple_of(place_ref[1] * 32, 32), 32), :]

    i, j = step // 4, lax.rem(step, 4)
    coupling = lax.dot_general(p_ref[i], p_ref[2 + j], (((0,), (0,)), ((), ())), preferred_element_type=F32)
    minus = (-coupling).astype(BF16)
    left = near_ref[:, 1, i].reshape(1024, 256)
    out_ref[0, 0] = jnp.dot(left, minus, preferred_element_type=F32).astype(BF16)


def panels(place, bucket_row, bucket_col, high, mid, near, far):
    smem = pl.BlockSpec(memory_space=pltpu.SMEM)
    full = lambda shape: pl.BlockSpec(shape, lambda s: (0,) * len(shape))
    return pl.pallas_call(
        panel_kernel,
        grid=(8,),
        out_shape=[
            jax.ShapeDtypeStruct((2, 128, 256), BF16),
            jax.ShapeDtypeStruct((4, 32, 256), BF16),
            jax.ShapeDtypeStruct((2, 4, 1024, 256), BF16),
        ],
        in_specs=[smem, smem, smem, full(high.shape), full(mid.shape), full(near.shape), full(far.shape)],
        out_specs=[
            full((2, 128, 256)),
            full((4, 32, 256)),
            pl.BlockSpec((1, 1, 1024, 256), lambda s: (s // 4, lax.rem(s, 4), 0, 0)),
        ],
        scratch_shapes=[pltpu.VMEM((6, 1024, 256), BF16)],
        compiler_params=pltpu.CompilerParams(vmem_limit_bytes=40 * 1024 * 1024),
        cost_estimate=pl.CostEstimate(flops=7 * 10**9, bytes_accessed=12 * 2**20, transcendentals=0),
        name="panels",
    )(place, bucket_row, bucket_col, high, mid, near, far)


def sent_to_all(array, axis):
    copies = jnp.broadcast_to(array, (lax.axis_size(axis), *array.shape))
    return lax.all_to_all(copies, axis, split_axis=0, concat_axis=0, tiled=True)


def per_device(diag_tile, left_row, right_row, right_col, bucket_row, bucket_col):
    zl, y, core = (lax.axis_index(axis) for axis in ROW)
    group = 2 * zl + y // 2
    wide = jnp.concatenate([diag_tile, diag_tile[:, :512]], axis=1)
    wide = jnp.concatenate([wide, diag_tile[:, 512:]], axis=1)
    part = lax.dynamic_slice_in_dim(wide, group * 128, SENT * 128, 1)
    part = sent_to_all(part, ("zl", "zh"))
    part = sent_to_all(part, ("y", "x"))
    other = lax.ppermute(part, "c", [(0, 1), (1, 0)])
    near = jnp.stack([right_row, left_row]).transpose(0, 2, 1, 3)
    far = right_col.transpose(1, 0, 2)
    part, other, near, far = lax.optimization_barrier((part, other, near, far))
    near = sent_to_all(near, COL)
    far = sent_to_all(far, ROW)
    high, mid = chol_inverse(core[None], part, other)
    place = jnp.stack([lax.axis_index(COL), lax.axis_index(ROW)])
    panel_row, panel_col, update_left = panels(place, bucket_row, bucket_col, high, mid, near, far)
    return panel_row.transpose(1, 0, 2), panel_col.transpose(1, 0, 2), update_left


def solution(mesh):
    fine = Mesh(mesh.devices.reshape(4, 4, 2, 4, 2), AXES)
    return jax.shard_map(
        per_device,
        mesh=fine,
        in_specs=(
            P(AXES, None),
            P(COL, ROW, None),
            P(COL, ROW, None),
            P(ROW, COL, None),
            P(ROW),
            P(COL),
        ),
        out_specs=(P(COL, ROW, None), P(ROW, COL, None), P(ROW, COL, None, None)),
        check_vma=False,
    )
```

```python
import functools

import jax
import jax.numpy as jnp
from jax import lax
from jax.experimental import pallas as pl
from jax.experimental.pallas import tpu as pltpu
from jax.sharding import Mesh
from jax.sharding import PartitionSpec as P


RSTEP = 64
F32 = jnp.float32
BF16 = jnp.bfloat16
AXES = ("zl", "y", "c", "x", "zh")
ROW = ("zl", "y", "c")
COL = ("x", "zh")
SENT = 5


def split3(x):
    high = x.astype(BF16)
    rest = x - high.astype(F32)
    middle = rest.astype(BF16)
    low = (rest - middle.astype(F32)).astype(BF16)
    return high, middle, low


def lane_copy(x, lane):
    return jnp.broadcast_to(x[:, lane : lane + 1], (8, 128))


def row_copy(x, row):
    return jnp.broadcast_to(x[row : row + 1, :], (8, 128))


def factor(groups):
    lane = lax.broadcasted_iota(jnp.int32, (8, 128), 1)
    sub = lax.broadcasted_iota(jnp.int32, (8, 128), 0)
    groups = list(groups)
    spread = lambda g, j: [lane_copy(groups[g], 8 * j + c) for c in range(8)]
    own = spread(0, 0)
    for j in range(16):
        below = {g: spread(g, j) for g in range(j + 1, 16)}
        following = spread(j + 1, j + 1) if j < 15 else None
        here = (lane >= 8 * j) & (lane < 8 * j + 8)
        x = jnp.where(here, jnp.where(lane - 8 * j == sub, 1.0, 0.0), groups[j])
        scales, rows, across = [], [], []
        for c in range(8):
            scale = lax.rsqrt(row_copy(own[c], c))
            column = own[c] * scale
            row = row_copy(x, c) * scale
            x = jnp.where(sub == c, row, x) - jnp.where(sub > c, column, 0.0) * row
            lower = {d: row_copy(column, d) for d in range(c + 1, 8)}
            for d in range(c + 1, 8):
                own[d] = own[d] - column * lower[d]
            scales.append(scale)
            rows.append(row)
            across.append(lower)
        groups[j] = x
        solved = [None] * 8
        for c in range(7, -1, -1):
            row = rows[c]
            for d in range(7, c, -1):
                row = row - across[c][d] * solved[d]
            solved[c] = row * scales[c]
        for g in range(j + 1, 16):
            cols = below[g]
            w = jnp.where(here, 0.0, groups[g])
            for c in range(8):
                if g > j + 2:
                    w = w - cols[c] * solved[c]
                    continue
                column = cols[c] * scales[c]
                for d in range(c + 1, 8):
                    cols[d] = cols[d] - column * across[c][d]
                w = w - column * rows[c]
                if g == j + 1:
                    following = [following[d] - column * row_copy(column, d) for d in range(8)]
            groups[g] = w
        own = following
    return groups


def dot6(left, right, dims=((1,), (0,))):
    (lh, lm, ll), (rh, rm, rl) = left, right
    dot = functools.partial(lax.dot_general, dimension_numbers=(dims, ((), ())), preferred_element_type=F32)
    lk, rk = dims[0][0], dims[1][0]
    join = lambda a, b, d: jnp.concatenate([a, b], axis=d)
    return (
        dot(join(lh, lm, lk), join(rh, rm, rk))
        + dot(join(lh, lm, lk), join(rm, rh, rk))
        + dot(join(lh, ll, lk), join(rl, rh, rk))
    )


def long_dot6(left, right):
    m = left.shape[0] // 3
    dot = functools.partial(jnp.dot, preferred_element_type=F32)
    a, b, c = dot(left, right[0]), dot(left[: 2 * m], right[1]), dot(left[:m], right[2])
    return a[:m] + (a[m : 2 * m] + b[:m]) + (b[m:] + (a[2 * m :] + c))


def chol_kernel(
    core_ref, mine_ref, other_ref, out_high_ref, out_mid_ref,
    row_ref, high_ref, mid_ref, low_ref, ls_ref, diag_ref, dh_ref, dm_ref, dl_ref, a_ref, sems,
):
    lane = lax.broadcasted_iota(jnp.int32, (128, 128), 1)
    sub = lax.broadcasted_iota(jnp.int32, (128, 128), 0)
    col = lax.broadcasted_iota(jnp.int32, (128, 1024), 1)
    xs_refs = (high_ref, mid_ref, low_ref)
    ds_refs = (dh_ref, dm_ref, dl_ref)
    for ref in (*xs_refs, ls_ref, *ds_refs, row_ref):
        ref[...] = jnp.zeros_like(ref)
    core = core_ref[0]
    for y in range(4):
        for x in range(4):
            for z in range(4):
                group = z * 2 + y // 2
                for part_ref, half in ((mine_ref, core), (other_ref, 1 - core)):
                    rows = pl.ds(pl.multiple_of(z * 256 + y * 64 + x * 8 + half * 32, 8), 8)
                    for m in range(SENT):
                        block = (group + m) % 8
                        if m == 4 and block < group:
                            continue
                        lanes = slice(128 * m, 128 * m + 128)
                        pieces = [part_ref[4 * y + x, 2 * z + end, :, lanes] for end in range(2)]
                        a_ref[rows, 128 * block : 128 * block + 128] = jnp.concatenate(pieces, axis=0)
    for group in range(5, 8):
        for block in range(group - 4):
            a_ref[128 * block : 128 * block + 128, 128 * group : 128 * group + 128] = jnp.transpose(
                a_ref[128 * group : 128 * group + 128, 128 * block : 128 * block + 128], (1, 0)
            )
    diag_ref[...] = a_ref[0:128, 0:128]

    def settle(at):
        for ref in xs_refs:
            ref[:, pl.ds(at, 128)] = jnp.zeros((1024, 128), BF16)
        row_ref[:, pl.ds(at, 128)] = jnp.where(lane == sub, 1.0, 0.0)
        x = dot6(tuple(ref[...] for ref in ds_refs), split3(row_ref[...]))
        for ref, part in zip(xs_refs, split3(x)):
            ref[pl.ds(at, 128), :] = part
        return x

    def step(depth, k, _):
        at = pl.multiple_of(k * 128, 128)
        before = pl.multiple_of(lax.rem(k + 7, 8) * 128, 128)
        after = pl.multiple_of(lax.rem(k + 1, 8) * 128, 128)
        groups = factor([diag_ref[8 * g : 8 * g + 8, :] for g in range(16)])
        inv = split3(jnp.where(lane <= sub, jnp.concatenate(groups, axis=0), 0.0))
        x = settle(before)
        for n, part in enumerate(split3(jnp.transpose(x, (1, 0)))):
            for g in range(8):
                ls_ref[g, 128 * n : 128 * n + 128, pl.ds(before, 128)] = part[128 * g : 128 * g + 128]
        upd = long_dot6(ls_ref[k, :, :depth], tuple(ref[:depth, :] for ref in xs_refs))
        row_ref[...] = jnp.where(col >= at, a_ref[pl.ds(at, 128), :], 0.0) - upd
        ahead = a_ref[pl.ds(after, 128), pl.ds(after, 128)] - long_dot6(
            ls_ref[lax.rem(k + 1, 8), :, :depth], tuple(ref[:depth, pl.ds(after, 128)] for ref in xs_refs)
        )
        side_t = split3(jnp.transpose(row_ref[:, pl.ds(after, 128)], (1, 0)))
        for ref, part in zip(ds_refs, inv):
            ref[...] = part
        xt = split3(dot6(side_t, inv, ((1,), (1,))))
        diag_ref[...] = ahead - dot6(xt, xt, ((1,), (1,)))
        return 0

    lax.fori_loop(0, 5, functools.partial(step, 512), 0)
    lax.fori_loop(5, 8, functools.partial(step, 1024), 0)
    settle(896)
    copies = [
        pltpu.make_async_copy(high_ref, out_high_ref, sems.at[0]),
        pltpu.make_async_copy(mid_ref, out_mid_ref, sems.at[1]),
    ]
    for copy in copies:
        copy.start()
    for copy in copies:
        copy.wait()


def chol_inverse(core, mine, other):
    n = 1024
    whole = pl.BlockSpec(memory_space=pltpu.VMEM)
    return pl.pallas_call(
        chol_kernel,
        out_shape=[jax.ShapeDtypeStruct((n, n), BF16)] * 2,
        in_specs=[pl.BlockSpec(memory_space=pltpu.SMEM), whole, whole],
        out_specs=[pl.BlockSpec(memory_space=pl.ANY)] * 2,
        scratch_shapes=[
            pltpu.VMEM((128, n), F32),
            *[pltpu.VMEM((n, n), BF16)] * 3,
            pltpu.VMEM((8, 384, n), BF16),
            pltpu.VMEM((128, 128), F32),
            *[pltpu.VMEM((128, 128), BF16)] * 3,
            pltpu.VMEM((n, n), F32),
            pltpu.SemaphoreType.DMA((2,)),
        ],
        compiler_params=pltpu.CompilerParams(vmem_limit_bytes=66_000_000),
        cost_estimate=pl.CostEstimate(flops=20 * 10**9, bytes_accessed=8 * 2**20, transcendentals=0),
        name="chol_inverse",
    )(core, mine, other)


def panel_kernel(
    place_ref, row_ref, col_ref, high_ref, mid_ref, near0_ref, near1_ref, near2_ref, near3_ref, far_ref,
    pr_ref, pc_ref, out_ref, p_ref, near_ref,
):
    lane = lax.broadcasted_iota(jnp.int32, (256, 256), 1)
    step = pl.program_id(0)

    @pl.when(step == 0)
    def _():
        for s, ref in enumerate((near0_ref, near1_ref, near2_ref, near3_ref)):
            source = lax.rem(place_ref[2] + 4 - s, 4)
            for q in range(2):
                end = place_ref[3] if q == 0 else 1 - place_ref[3]
                rows = pl.ds(pl.multiple_of(source * 256 + end * 128, 128), 128)
                for kind in range(2):
                    for t in range(2):
                        near_ref[2 * kind + t, rows, :] = ref[q, kind, t]
        for i in range(4):
            depth = 256 * (i + 1)
            rows = slice(256 * i, depth)
            high, mid = high_ref[rows, :depth], mid_ref[rows, :depth]
            for t in range(6):
                if t < 2:
                    right = near_ref[t, :depth, :]
                    live = RSTEP * row_ref[t]
                else:
                    right = far_ref[: depth // 32, t - 2].reshape(depth, 256)
                    live = RSTEP * col_ref[t - 2]
                solved = jnp.dot(high, right, preferred_element_type=F32)
                solved = solved + jnp.dot(mid, right, preferred_element_type=F32)
                p_ref[t, rows, :] = jnp.where(lane < live, solved, 0.0).astype(BF16)
        for t in range(2):
            pr_ref[t] = p_ref[t, pl.ds(pl.multiple_of(place_ref[0] * 128, 128), 128), :]
        for t in range(4):
            pc_ref[t] = p_ref[2 + t, pl.ds(pl.multiple_of(place_ref[1] * 32, 32), 32), :]

    i, j = step // 4, lax.rem(step, 4)
    coupling = lax.dot_general(p_ref[i], p_ref[2 + j], (((0,), (0,)), ((), ())), preferred_element_type=F32)
    minus = (-coupling).astype(BF16)
    out_ref[0, 0] = jnp.dot(near_ref[2 + i], minus, preferred_element_type=F32).astype(BF16)


def panels(place, bucket_row, bucket_col, high, mid, near, far):
    smem = pl.BlockSpec(memory_space=pltpu.SMEM)
    full = lambda shape: pl.BlockSpec(shape, lambda s: (0,) * len(shape))
    arrays = (high, mid, *near, far)
    return pl.pallas_call(
        panel_kernel,
        grid=(8,),
        out_shape=[
            jax.ShapeDtypeStruct((2, 128, 256), BF16),
            jax.ShapeDtypeStruct((4, 32, 256), BF16),
            jax.ShapeDtypeStruct((2, 4, 1024, 256), BF16),
        ],
        in_specs=[smem, smem, smem, *[full(array.shape) for array in arrays]],
        out_specs=[
            full((2, 128, 256)),
            full((4, 32, 256)),
            pl.BlockSpec((1, 1, 1024, 256), lambda s: (s // 4, lax.rem(s, 4), 0, 0)),
        ],
        scratch_shapes=[pltpu.VMEM((6, 1024, 256), BF16), pltpu.VMEM((4, 1024, 256), BF16)],
        compiler_params=pltpu.CompilerParams(vmem_limit_bytes=66_000_000),
        cost_estimate=pl.CostEstimate(flops=7 * 10**9, bytes_accessed=12 * 2**20, transcendentals=0),
        name="panels",
    )(place, bucket_row, bucket_col, *arrays)


def moved(array, axis, by):
    count = lax.axis_size(axis)
    return lax.ppermute(array, axis, [(k, (k + by) % count) for k in range(count)])


def sent_to_all(array, axis):
    copies = jnp.broadcast_to(array, (lax.axis_size(axis), *array.shape))
    return lax.all_to_all(copies, axis, split_axis=0, concat_axis=0, tiled=True)


def per_device(diag_tile, left_row, right_row, right_col, bucket_row, bucket_col):
    zl, y, core = (lax.axis_index(axis) for axis in ROW)
    group = 2 * zl + y // 2
    wide = jnp.concatenate([diag_tile, diag_tile[:, :512]], axis=1)
    wide = jnp.concatenate([wide, diag_tile[:, 512:]], axis=1)
    part = lax.dynamic_slice_in_dim(wide, group * 128, SENT * 128, 1)
    near = jnp.stack([right_row, left_row]).transpose(0, 2, 1, 3)
    swapped = moved(near, "zh", 1)
    part = sent_to_all(part, ("zl", "zh"))
    part = sent_to_all(part, ("y", "x"))
    near = jnp.stack([near, swapped])
    other = moved(part, "c", 1)
    far = right_col.transpose(1, 0, 2)
    part, other, near, far = lax.optimization_barrier((part, other, near, far))
    far = sent_to_all(far, ROW)
    near = [near, *[moved(near, "x", by) for by in range(1, 4)]]
    high, mid = chol_inverse(core[None], part, other)
    place = jnp.stack([lax.axis_index(COL), lax.axis_index(ROW), lax.axis_index("x"), lax.axis_index("zh")])
    panel_row, panel_col, update_left = panels(place, bucket_row, bucket_col, high, mid, near, far)
    return panel_row.transpose(1, 0, 2), panel_col.transpose(1, 0, 2), update_left


def solution(mesh):
    fine = Mesh(mesh.devices.reshape(4, 4, 2, 4, 2), AXES)
    return jax.shard_map(
        per_device,
        mesh=fine,
        in_specs=(
            P(AXES, None),
            P(COL, ROW, None),
            P(COL, ROW, None),
            P(ROW, COL, None),
            P(ROW),
            P(COL),
        ),
        out_specs=(P(COL, ROW, None), P(ROW, COL, None), P(ROW, COL, None, None)),
        check_vma=False,
    )
```

```python
import functools

import jax
import jax.numpy as jnp
from jax import lax
from jax.experimental import pallas as pl
from jax.experimental.pallas import tpu as pltpu
from jax.sharding import Mesh
from jax.sharding import PartitionSpec as P


RSTEP = 64
F32 = jnp.float32
BF16 = jnp.bfloat16
AXES = ("zl", "y", "c", "x", "zh")
ROW = ("zl", "y", "c")
COL = ("x", "zh")
SENT = 5


def split3(x):
    high = x.astype(BF16)
    rest = x - high.astype(F32)
    middle = rest.astype(BF16)
    low = (rest - middle.astype(F32)).astype(BF16)
    return high, middle, low


def lane_copy(x, lane):
    return jnp.broadcast_to(x[:, lane : lane + 1], (8, 128))


def row_copy(x, row):
    return jnp.broadcast_to(x[row : row + 1, :], (8, 128))


def factor(groups, first):
    lane = lax.broadcasted_iota(jnp.int32, (8, 128), 1)
    sub = lax.broadcasted_iota(jnp.int32, (8, 128), 0)
    groups = dict(enumerate(groups, first))
    last = first + 8
    spread = lambda g, j: [lane_copy(groups[g], 8 * j + c) for c in range(8)]
    own = spread(first, first)
    for j in range(first, last):
        below = {g: spread(g, j) for g in range(j + 1, last)}
        following = spread(j + 1, j + 1) if j + 1 < last else None
        here = (lane >= 8 * j) & (lane < 8 * j + 8)
        x = jnp.where(here, jnp.where(lane - 8 * j == sub, 1.0, 0.0), groups[j])
        scales, rows, across = [], [], []
        pivot = row_copy(own[0], 0)
        for c in range(8):
            scale = lax.rsqrt(pivot)
            column = own[c] * scale
            lower = {d: row_copy(own[c], d) * scale for d in range(c + 1, 8)}
            if c < 7:
                pivot = row_copy(own[c + 1], c + 1) - lower[c + 1] * lower[c + 1]
            row = row_copy(x, c) * scale
            x = jnp.where(sub == c, row, x) - jnp.where(sub > c, column, 0.0) * row
            for d in range(c + 1, 8):
                own[d] = own[d] - column * lower[d]
            scales.append(scale)
            rows.append(row)
            across.append(lower)
        groups[j] = x
        solved = [None] * 8
        for c in range(7, -1, -1):
            row = rows[c]
            for d in range(7, c, -1):
                row = row - across[c][d] * solved[d]
            solved[c] = row * scales[c]
        for g in range(j + 1, last):
            cols = below[g]
            w = jnp.where(here, 0.0, groups[g])
            for c in range(8):
                if g > j + 2:
                    w = w - cols[c] * solved[c]
                    continue
                column = cols[c] * scales[c]
                for d in range(c + 1, 8):
                    cols[d] = cols[d] - column * across[c][d]
                w = w - column * rows[c]
                if g == j + 1:
                    following = [following[d] - column * row_copy(column, d) for d in range(8)]
            groups[g] = w
        own = following
    return jnp.concatenate([groups[g] for g in range(first, last)], axis=0)


def dot6(left, right, dims=((1,), (0,))):
    (lh, lm, ll), (rh, rm, rl) = left, right
    dot = functools.partial(lax.dot_general, dimension_numbers=(dims, ((), ())), preferred_element_type=F32)
    lk, rk = dims[0][0], dims[1][0]
    join = lambda a, b, d: jnp.concatenate([a, b], axis=d)
    return (
        dot(join(lh, lm, lk), join(rh, rm, rk))
        + dot(join(lh, lm, lk), join(rm, rh, rk))
        + dot(join(lh, ll, lk), join(rl, rh, rk))
    )


def long_dot6(left, right):
    m = left.shape[0] // 3
    dot = functools.partial(jnp.dot, preferred_element_type=F32)
    a, b, c = dot(left, right[0]), dot(left[: 2 * m], right[1]), dot(left[:m], right[2])
    return a[:m] + (a[m : 2 * m] + b[:m]) + (b[m:] + (a[2 * m :] + c))


def chol_kernel(
    core_ref, mine_ref, other_ref, out_high_ref, out_mid_ref,
    row_ref, high_ref, mid_ref, low_ref, ls_ref, diag_ref, dh_ref, dm_ref, dl_ref, a_ref, sems,
):
    lane = lax.broadcasted_iota(jnp.int32, (128, 128), 1)
    sub = lax.broadcasted_iota(jnp.int32, (128, 128), 0)
    col = lax.broadcasted_iota(jnp.int32, (128, 1024), 1)
    half_lane = lax.broadcasted_iota(jnp.int32, (64, 128), 1)
    half_sub = lax.broadcasted_iota(jnp.int32, (64, 128), 0)
    xs_refs = (high_ref, mid_ref, low_ref)
    ds_refs = (dh_ref, dm_ref, dl_ref)
    for ref in (*xs_refs, ls_ref, *ds_refs, row_ref):
        ref[...] = jnp.zeros_like(ref)
    core = core_ref[0]
    for y in range(4):
        for x in range(4):
            for z in range(4):
                group = z * 2 + y // 2
                for part_ref, half in ((mine_ref, core), (other_ref, 1 - core)):
                    rows = pl.ds(pl.multiple_of(z * 256 + y * 64 + x * 8 + half * 32, 8), 8)
                    for m in range(SENT):
                        block = (group + m) % 8
                        if m == 4 and block < group:
                            continue
                        lanes = slice(128 * m, 128 * m + 128)
                        pieces = [part_ref[4 * y + x, 2 * z + end, :, lanes] for end in range(2)]
                        a_ref[rows, 128 * block : 128 * block + 128] = jnp.concatenate(pieces, axis=0)
    for group in range(5, 8):
        for block in range(group - 4):
            a_ref[128 * block : 128 * block + 128, 128 * group : 128 * group + 128] = jnp.transpose(
                a_ref[128 * group : 128 * group + 128, 128 * block : 128 * block + 128], (1, 0)
            )
    diag_ref[...] = a_ref[0:128, 0:128]

    def settle(at):
        for ref in xs_refs:
            ref[:, pl.ds(at, 128)] = jnp.zeros((1024, 128), BF16)
        row_ref[:, pl.ds(at, 128)] = jnp.where(lane == sub, 1.0, 0.0)
        x = dot6(tuple(ref[...] for ref in ds_refs), split3(row_ref[...]))
        for ref, part in zip(xs_refs, split3(x)):
            ref[pl.ds(at, 128), :] = part
        return x

    def step(depth, k, _):
        at = pl.multiple_of(k * 128, 128)
        before = pl.multiple_of(lax.rem(k + 7, 8) * 128, 128)
        after = pl.multiple_of(lax.rem(k + 1, 8) * 128, 128)
        top = factor([diag_ref[8 * g : 8 * g + 8, :] for g in range(8)], 0)
        cross = split3(jnp.transpose(top, (1, 0))[64:, :])
        known = split3(jnp.where((half_lane <= half_sub) | (half_lane >= 64), top, 0.0))
        bottom = jnp.where(half_lane >= 64, diag_ref[64:, :], 0.0) - dot6(cross, known)
        bottom = factor([bottom[8 * g : 8 * g + 8, :] for g in range(8)], 8)
        halves = [
            split3(jnp.where(half_lane <= half_sub + 64 * n, rows, 0.0)) for n, rows in enumerate((top, bottom))
        ]
        x = settle(before)
        for n, part in enumerate(split3(jnp.transpose(x, (1, 0)))):
            for g in range(8):
                ls_ref[g, 128 * n : 128 * n + 128, pl.ds(before, 128)] = part[128 * g : 128 * g + 128]
        upd = long_dot6(ls_ref[k, :, :depth], tuple(ref[:depth, :] for ref in xs_refs))
        row_ref[...] = jnp.where(col >= at, a_ref[pl.ds(at, 128), :], 0.0) - upd
        ahead = a_ref[pl.ds(after, 128), pl.ds(after, 128)] - long_dot6(
            ls_ref[lax.rem(k + 1, 8), :, :depth], tuple(ref[:depth, pl.ds(after, 128)] for ref in xs_refs)
        )
        side_t = split3(jnp.transpose(row_ref[:, pl.ds(after, 128)], (1, 0)))
        for n, half in enumerate(halves):
            for ref, part in zip(ds_refs, half):
                ref[64 * n : 64 * n + 64, :] = part
            xt = split3(dot6(side_t, half, ((1,), (1,))))
            ahead = ahead - dot6(xt, xt, ((1,), (1,)))
        diag_ref[...] = ahead
        return 0

    lax.fori_loop(0, 5, functools.partial(step, 512), 0)
    lax.fori_loop(5, 8, functools.partial(step, 1024), 0)
    settle(896)
    copies = [
        pltpu.make_async_copy(high_ref, out_high_ref, sems.at[0]),
        pltpu.make_async_copy(mid_ref, out_mid_ref, sems.at[1]),
    ]
    for copy in copies:
        copy.start()
    for copy in copies:
        copy.wait()


def chol_inverse(core, mine, other):
    n = 1024
    whole = pl.BlockSpec(memory_space=pltpu.VMEM)
    return pl.pallas_call(
        chol_kernel,
        out_shape=[jax.ShapeDtypeStruct((n, n), BF16)] * 2,
        in_specs=[pl.BlockSpec(memory_space=pltpu.SMEM), whole, whole],
        out_specs=[pl.BlockSpec(memory_space=pl.ANY)] * 2,
        scratch_shapes=[
            pltpu.VMEM((128, n), F32),
            *[pltpu.VMEM((n, n), BF16)] * 3,
            pltpu.VMEM((8, 384, n), BF16),
            pltpu.VMEM((128, 128), F32),
            *[pltpu.VMEM((128, 128), BF16)] * 3,
            pltpu.VMEM((n, n), F32),
            pltpu.SemaphoreType.DMA((2,)),
        ],
        compiler_params=pltpu.CompilerParams(vmem_limit_bytes=66_000_000),
        cost_estimate=pl.CostEstimate(flops=20 * 10**9, bytes_accessed=8 * 2**20, transcendentals=0),
        name="chol_inverse",
    )(core, mine, other)


def panel_kernel(
    place_ref, row_ref, col_ref, high_ref, mid_ref, near0_ref, near1_ref, near2_ref, near3_ref, far_ref,
    pr_ref, pc_ref, out_ref, rows_ref, cols_ref, near_ref, minus_ref, inverse_ref, sems,
):
    lane = lax.broadcasted_iota(jnp.int32, (256, 256), 1)
    step = pl.program_id(0)

    @pl.when(step == 0)
    def _():
        copies = [
            pltpu.make_async_copy(ref.at[pl.ds(256 * i, 256), :], inverse_ref.at[i, n], sems.at[i, n])
            for i in range(4)
            for n, ref in enumerate((high_ref, mid_ref))
        ]
        for copy in copies:
            copy.start()
        for s, ref in enumerate((near0_ref, near1_ref, near2_ref, near3_ref)):
            source = lax.rem(place_ref[2] + 4 - s, 4)
            for q in range(2):
                end = place_ref[3] if q == 0 else 1 - place_ref[3]
                rows = pl.ds(pl.multiple_of(source * 256 + end * 128, 128), 128)
                for kind in range(2):
                    for t in range(2):
                        near_ref[2 * kind + t, rows, :] = ref[q, kind, t]
        for i in range(4):
            depth = 256 * (i + 1)
            rows = slice(256 * i, depth)
            copies[2 * i].wait()
            copies[2 * i + 1].wait()
            inverse = inverse_ref[i, :, :, :depth].reshape(512, depth)
            for t in range(6):
                if t < 2:
                    right = near_ref[t, :depth, :]
                    live = RSTEP * row_ref[t]
                else:
                    right = far_ref[: depth // 32, t - 2].reshape(depth, 256)
                    live = RSTEP * col_ref[t - 2]
                solved = jnp.dot(inverse, right, preferred_element_type=F32)
                solved = jnp.where(lane < live, solved[:256] + solved[256:], 0.0).astype(BF16)
                if t < 2:
                    rows_ref[t, rows, :] = solved
                else:
                    cols_ref[rows, 256 * t - 512 : 256 * t - 256] = solved
        mine = pl.ds(pl.multiple_of(place_ref[0] * 128, 128), 128)
        for t in range(2):
            pr_ref[t] = rows_ref[t, mine, :]
        mine = pl.ds(pl.multiple_of(place_ref[1] * 32, 32), 32)
        for t in range(4):
            pc_ref[t] = cols_ref[mine, 256 * t : 256 * t + 256]
        for i in range(2):
            coupling = lax.dot_general(
                rows_ref[i], cols_ref[...], (((0,), (0,)), ((), ())), preferred_element_type=F32
            )
            for t in range(4):
                minus_ref[4 * i + t] = (-coupling[:, 256 * t : 256 * t + 256]).astype(BF16)

    out_ref[0, 0] = jnp.dot(near_ref[2 + step // 4], minus_ref[step], preferred_element_type=F32).astype(BF16)


def panels(place, bucket_row, bucket_col, high, mid, near, far):
    smem = pl.BlockSpec(memory_space=pltpu.SMEM)
    full = lambda shape: pl.BlockSpec(shape, lambda s: (0,) * len(shape))
    arrays = (high, mid, *near, far)
    return pl.pallas_call(
        panel_kernel,
        grid=(8,),
        out_shape=[
            jax.ShapeDtypeStruct((2, 128, 256), BF16),
            jax.ShapeDtypeStruct((4, 32, 256), BF16),
            jax.ShapeDtypeStruct((2, 4, 1024, 256), BF16),
        ],
        in_specs=[smem, smem, smem, *[pl.BlockSpec(memory_space=pl.ANY)] * 2, *[full(array.shape) for array in arrays[2:]]],
        out_specs=[
            full((2, 128, 256)),
            full((4, 32, 256)),
            pl.BlockSpec((1, 1, 1024, 256), lambda s: (s // 4, lax.rem(s, 4), 0, 0)),
        ],
        scratch_shapes=[
            pltpu.VMEM((2, 1024, 256), BF16),
            pltpu.VMEM((1024, 1024), BF16),
            pltpu.VMEM((4, 1024, 256), BF16),
            pltpu.VMEM((8, 256, 256), BF16),
            pltpu.VMEM((4, 2, 256, 1024), BF16),
            pltpu.SemaphoreType.DMA((4, 2)),
        ],
        compiler_params=pltpu.CompilerParams(vmem_limit_bytes=66_000_000),
        cost_estimate=pl.CostEstimate(flops=7 * 10**9, bytes_accessed=12 * 2**20, transcendentals=0),
        name="panels",
    )(place, bucket_row, bucket_col, *arrays)


def moved(array, axis, by):
    count = lax.axis_size(axis)
    return lax.ppermute(array, axis, [(k, (k + by) % count) for k in range(count)])


def copies_for(array, axis):
    return jnp.broadcast_to(array, (lax.axis_size(axis), *array.shape))


def exchanged(copies, axis):
    return lax.all_to_all(copies, axis, split_axis=0, concat_axis=0, tiled=True)


def sent_to_all(array, axis):
    return exchanged(copies_for(array, axis), axis)


def per_device(diag_tile, left_row, right_row, right_col, bucket_row, bucket_col):
    zl, y, core = (lax.axis_index(axis) for axis in ROW)
    group = 2 * zl + y // 2
    wide = jnp.concatenate([diag_tile, diag_tile[:, :512]], axis=1)
    wide = jnp.concatenate([wide, diag_tile[:, 512:]], axis=1)
    part = lax.dynamic_slice_in_dim(wide, group * 128, SENT * 128, 1)
    near = jnp.stack([right_row, left_row]).transpose(0, 2, 1, 3)
    swapped = moved(near, "zh", 1)
    part = sent_to_all(part, ("zl", "zh"))
    part = sent_to_all(part, ("y", "x"))
    near = jnp.stack([near, swapped])
    other = moved(part, "c", 1)
    far = copies_for(right_col.transpose(1, 0, 2), ROW)
    part, other, near, far = lax.optimization_barrier((part, other, near, far))
    far = exchanged(far, ROW)
    near = [near, *[moved(near, "x", by) for by in range(1, 4)]]
    high, mid = chol_inverse(core[None], part, other)
    place = jnp.stack([lax.axis_index(COL), lax.axis_index(ROW), lax.axis_index("x"), lax.axis_index("zh")])
    panel_row, panel_col, update_left = panels(place, bucket_row, bucket_col, high, mid, near, far)
    return panel_row.transpose(1, 0, 2), panel_col.transpose(1, 0, 2), update_left


def solution(mesh):
    fine = Mesh(mesh.devices.reshape(4, 4, 2, 4, 2), AXES)
    return jax.shard_map(
        per_device,
        mesh=fine,
        in_specs=(
            P(AXES, None),
            P(COL, ROW, None),
            P(COL, ROW, None),
            P(ROW, COL, None),
            P(ROW),
            P(COL),
        ),
        out_specs=(P(COL, ROW, None), P(ROW, COL, None), P(ROW, COL, None, None)),
        check_vma=False,
    )
```

```python
import functools

import jax
import jax.numpy as jnp
from jax import lax
from jax.experimental import pallas as pl
from jax.experimental.pallas import tpu as pltpu
from jax.sharding import Mesh
from jax.sharding import PartitionSpec as P


RSTEP = 64
F32 = jnp.float32
BF16 = jnp.bfloat16
AXES = ("zl", "y", "c", "x", "zh")
ROW = ("zl", "y", "c")
COL = ("x", "zh")
SENT = 5


def split3(x):
    high = x.astype(BF16)
    rest = x - high.astype(F32)
    middle = rest.astype(BF16)
    low = (rest - middle.astype(F32)).astype(BF16)
    return high, middle, low


def lane_copy(x, lane):
    return jnp.broadcast_to(x[:, lane : lane + 1], (8, 128))


def row_copy(x, row):
    return jnp.broadcast_to(x[row : row + 1, :], (8, 128))


def factor(groups, first):
    lane = lax.broadcasted_iota(jnp.int32, (8, 128), 1)
    sub = lax.broadcasted_iota(jnp.int32, (8, 128), 0)
    groups = dict(enumerate(groups, first))
    last = first + 8
    spread = lambda g, j: [lane_copy(groups[g], 8 * j + c) for c in range(8)]
    own = spread(first, first)
    for j in range(first, last):
        below = {g: spread(g, j) for g in range(j + 1, last)}
        following = spread(j + 1, j + 1) if j + 1 < last else None
        here = (lane >= 8 * j) & (lane < 8 * j + 8)
        x = jnp.where(here, jnp.where(lane - 8 * j == sub, 1.0, 0.0), groups[j])
        scales, rows, across = [], [], []
        pivot = row_copy(own[0], 0)
        for c in range(8):
            scale = lax.rsqrt(pivot)
            column = own[c] * scale
            lower = {d: row_copy(own[c], d) * scale for d in range(c + 1, 8)}
            if c < 7:
                pivot = row_copy(own[c + 1], c + 1) - lower[c + 1] * lower[c + 1]
            row = row_copy(x, c) * scale
            x = jnp.where(sub == c, row, x) - jnp.where(sub > c, column, 0.0) * row
            for d in range(c + 1, 8):
                own[d] = own[d] - column * lower[d]
            scales.append(scale)
            rows.append(row)
            across.append(lower)
        groups[j] = x
        solved = [None] * 8
        for c in range(7, -1, -1):
            row = rows[c]
            for d in range(7, c, -1):
                row = row - across[c][d] * solved[d]
            solved[c] = row * scales[c]
        for g in range(j + 1, last):
            cols = below[g]
            w = jnp.where(here, 0.0, groups[g])
            for c in range(8):
                if g > j + 2:
                    w = w - cols[c] * solved[c]
                    continue
                column = cols[c] * scales[c]
                for d in range(c + 1, 8):
                    cols[d] = cols[d] - column * across[c][d]
                w = w - column * rows[c]
                if g == j + 1:
                    following = [following[d] - column * row_copy(column, d) for d in range(8)]
            groups[g] = w
        own = following
    return jnp.concatenate([groups[g] for g in range(first, last)], axis=0)


def dot6(left, right, dims=((1,), (0,))):
    (lh, lm, ll), (rh, rm, rl) = left, right
    dot = functools.partial(lax.dot_general, dimension_numbers=(dims, ((), ())), preferred_element_type=F32)
    lk, rk = dims[0][0], dims[1][0]
    join = lambda a, b, d: jnp.concatenate([a, b], axis=d)
    return (
        dot(join(lh, lm, lk), join(rh, rm, rk))
        + dot(join(lh, lm, lk), join(rm, rh, rk))
        + dot(join(lh, ll, lk), join(rl, rh, rk))
    )


def long_dot6(left, right):
    m = left.shape[0] // 3
    dot = functools.partial(jnp.dot, preferred_element_type=F32)
    a, b, c = dot(left, right[0]), dot(left[: 2 * m], right[1]), dot(left[:m], right[2])
    return a[:m] + (a[m : 2 * m] + b[:m]) + (b[m:] + (a[2 * m :] + c))


def chol_kernel(
    core_ref, mine_ref, other_ref, out_high_ref, out_mid_ref,
    row_ref, high_ref, mid_ref, low_ref, ls_ref, diag_ref, dh_ref, dm_ref, dl_ref, a_ref, sems,
):
    lane = lax.broadcasted_iota(jnp.int32, (128, 128), 1)
    sub = lax.broadcasted_iota(jnp.int32, (128, 128), 0)
    col = lax.broadcasted_iota(jnp.int32, (128, 1024), 1)
    half_lane = lax.broadcasted_iota(jnp.int32, (64, 128), 1)
    half_sub = lax.broadcasted_iota(jnp.int32, (64, 128), 0)
    xs_refs = (high_ref, mid_ref, low_ref)
    ds_refs = (dh_ref, dm_ref, dl_ref)
    for ref in (*xs_refs, ls_ref, *ds_refs, row_ref):
        ref[...] = jnp.zeros_like(ref)
    core = core_ref[0]
    for y in range(4):
        for x in range(4):
            for z in range(4):
                group = z * 2 + y // 2
                for part_ref, half in ((mine_ref, core), (other_ref, 1 - core)):
                    rows = pl.ds(pl.multiple_of(z * 256 + y * 64 + x * 8 + half * 32, 8), 8)
                    for m in range(SENT):
                        block = (group + m) % 8
                        if m == 4 and block < group:
                            continue
                        lanes = slice(128 * m, 128 * m + 128)
                        pieces = [part_ref[4 * y + x, 2 * z + end, :, lanes] for end in range(2)]
                        a_ref[rows, 128 * block : 128 * block + 128] = jnp.concatenate(pieces, axis=0)
    for group in range(5, 8):
        for block in range(group - 4):
            a_ref[128 * block : 128 * block + 128, 128 * group : 128 * group + 128] = jnp.transpose(
                a_ref[128 * group : 128 * group + 128, 128 * block : 128 * block + 128], (1, 0)
            )
    diag_ref[...] = a_ref[0:128, 0:128]

    def settle(at):
        for ref in xs_refs:
            ref[:, pl.ds(at, 128)] = jnp.zeros((1024, 128), BF16)
        row_ref[:, pl.ds(at, 128)] = jnp.where(lane == sub, 1.0, 0.0)
        x = dot6(tuple(ref[...] for ref in ds_refs), split3(row_ref[...]))
        for ref, part in zip(xs_refs, split3(x)):
            ref[pl.ds(at, 128), :] = part
        return x

    def step(depth, k, _):
        at = pl.multiple_of(k * 128, 128)
        before = pl.multiple_of(lax.rem(k + 7, 8) * 128, 128)
        after = pl.multiple_of(lax.rem(k + 1, 8) * 128, 128)
        top = factor([diag_ref[8 * g : 8 * g + 8, :] for g in range(8)], 0)
        cross = split3(jnp.transpose(top, (1, 0))[64:, :])
        known = split3(jnp.where((half_lane <= half_sub) | (half_lane >= 64), top, 0.0))
        bottom = jnp.where(half_lane >= 64, diag_ref[64:, :], 0.0) - dot6(cross, known)
        bottom = factor([bottom[8 * g : 8 * g + 8, :] for g in range(8)], 8)
        halves = [
            split3(jnp.where(half_lane <= half_sub + 64 * n, rows, 0.0)) for n, rows in enumerate((top, bottom))
        ]
        x = settle(before)
        for n, part in enumerate(split3(jnp.transpose(x, (1, 0)))):
            for g in range(8):
                ls_ref[g, 128 * n : 128 * n + 128, pl.ds(before, 128)] = part[128 * g : 128 * g + 128]
        upd = long_dot6(ls_ref[k, :, :depth], tuple(ref[:depth, :] for ref in xs_refs))
        row_ref[...] = jnp.where(col >= at, a_ref[pl.ds(at, 128), :], 0.0) - upd
        ahead = a_ref[pl.ds(after, 128), pl.ds(after, 128)] - long_dot6(
            ls_ref[lax.rem(k + 1, 8), :, :depth], tuple(ref[:depth, pl.ds(after, 128)] for ref in xs_refs)
        )
        side_t = split3(jnp.transpose(row_ref[:, pl.ds(after, 128)], (1, 0)))
        for n, half in enumerate(halves):
            for ref, part in zip(ds_refs, half):
                ref[64 * n : 64 * n + 64, :] = part
            xt = split3(dot6(side_t, half, ((1,), (1,))))
            ahead = ahead - dot6(xt, xt, ((1,), (1,)))
        diag_ref[...] = ahead
        return 0

    lax.fori_loop(0, 5, functools.partial(step, 512), 0)
    lax.fori_loop(5, 8, functools.partial(step, 1024), 0)
    settle(896)
    copies = [
        pltpu.make_async_copy(high_ref, out_high_ref, sems.at[0]),
        pltpu.make_async_copy(mid_ref, out_mid_ref, sems.at[1]),
    ]
    for copy in copies:
        copy.start()
    for copy in copies:
        copy.wait()


def chol_inverse(core, mine, other):
    n = 1024
    whole = pl.BlockSpec(memory_space=pltpu.VMEM)
    return pl.pallas_call(
        chol_kernel,
        out_shape=[jax.ShapeDtypeStruct((n, n), BF16)] * 2,
        in_specs=[pl.BlockSpec(memory_space=pltpu.SMEM), whole, whole],
        out_specs=[pl.BlockSpec(memory_space=pl.ANY)] * 2,
        scratch_shapes=[
            pltpu.VMEM((128, n), F32),
            *[pltpu.VMEM((n, n), BF16)] * 3,
            pltpu.VMEM((8, 384, n), BF16),
            pltpu.VMEM((128, 128), F32),
            *[pltpu.VMEM((128, 128), BF16)] * 3,
            pltpu.VMEM((n, n), F32),
            pltpu.SemaphoreType.DMA((2,)),
        ],
        compiler_params=pltpu.CompilerParams(vmem_limit_bytes=66_000_000),
        cost_estimate=pl.CostEstimate(flops=20 * 10**9, bytes_accessed=8 * 2**20, transcendentals=0),
        name="chol_inverse",
    )(core, mine, other)


def panel_kernel(
    place_ref, row_ref, col_ref, high_ref, mid_ref, near0_ref, near1_ref, near2_ref, near3_ref, own_ref, twin_ref,
    pr_ref, pc_ref, out_ref, rows_ref, cols_ref, near_ref, far_ref, minus_ref, inverse_ref, sems,
):
    lane = lax.broadcasted_iota(jnp.int32, (256, 256), 1)
    step = pl.program_id(0)

    @pl.when(step == 0)
    def _():
        copies = [
            pltpu.make_async_copy(ref.at[pl.ds(256 * i, 256), :], inverse_ref.at[i, n], sems.at[i, n])
            for i in range(4)
            for n, ref in enumerate((high_ref, mid_ref))
        ]
        for copy in copies:
            copy.start()
        for s, ref in enumerate((near0_ref, near1_ref, near2_ref, near3_ref)):
            source = lax.rem(place_ref[2] + 4 - s, 4)
            for q in range(2):
                end = place_ref[3] if q == 0 else 1 - place_ref[3]
                rows = pl.ds(pl.multiple_of(source * 256 + end * 128, 128), 128)
                for kind in range(2):
                    for t in range(2):
                        near_ref[2 * kind + t, rows, :] = ref[q, kind, t]
        for core, ref in ((place_ref[4], own_ref), (1 - place_ref[4], twin_ref)):
            for k in range(16):
                rows = pl.ds(pl.multiple_of(64 * k + 32 * core, 32), 32)
                for t in range(4):
                    far_ref[t, rows, :] = ref[k, t]
        for i in range(4):
            depth = 256 * (i + 1)
            rows = slice(256 * i, depth)
            copies[2 * i].wait()
            copies[2 * i + 1].wait()
            inverse = inverse_ref[i, :, :, :depth].reshape(512, depth)
            for t in range(6):
                if t < 2:
                    right = near_ref[t, :depth, :]
                    live = RSTEP * row_ref[t]
                else:
                    right = far_ref[t - 2, :depth, :]
                    live = RSTEP * col_ref[t - 2]
                solved = jnp.dot(inverse, right, preferred_element_type=F32)
                solved = jnp.where(lane < live, solved[:256] + solved[256:], 0.0).astype(BF16)
                if t < 2:
                    rows_ref[t, rows, :] = solved
                else:
                    cols_ref[rows, 256 * t - 512 : 256 * t - 256] = solved
        mine = pl.ds(pl.multiple_of(place_ref[0] * 128, 128), 128)
        for t in range(2):
            pr_ref[t] = rows_ref[t, mine, :]
        mine = pl.ds(pl.multiple_of(place_ref[1] * 32, 32), 32)
        for t in range(4):
            pc_ref[t] = cols_ref[mine, 256 * t : 256 * t + 256]
        for i in range(2):
            coupling = lax.dot_general(
                rows_ref[i], cols_ref[...], (((0,), (0,)), ((), ())), preferred_element_type=F32
            )
            for t in range(4):
                minus_ref[4 * i + t] = (-coupling[:, 256 * t : 256 * t + 256]).astype(BF16)

    out_ref[0, 0] = jnp.dot(near_ref[2 + step // 4], minus_ref[step], preferred_element_type=F32).astype(BF16)


def panels(place, bucket_row, bucket_col, high, mid, near, far):
    smem = pl.BlockSpec(memory_space=pltpu.SMEM)
    full = lambda shape: pl.BlockSpec(shape, lambda s: (0,) * len(shape))
    arrays = (high, mid, *near, *far)
    return pl.pallas_call(
        panel_kernel,
        grid=(8,),
        out_shape=[
            jax.ShapeDtypeStruct((2, 128, 256), BF16),
            jax.ShapeDtypeStruct((4, 32, 256), BF16),
            jax.ShapeDtypeStruct((2, 4, 1024, 256), BF16),
        ],
        in_specs=[smem, smem, smem, *[pl.BlockSpec(memory_space=pl.ANY)] * 2, *[full(array.shape) for array in arrays[2:]]],
        out_specs=[
            full((2, 128, 256)),
            full((4, 32, 256)),
            pl.BlockSpec((1, 1, 1024, 256), lambda s: (s // 4, lax.rem(s, 4), 0, 0)),
        ],
        scratch_shapes=[
            pltpu.VMEM((2, 1024, 256), BF16),
            pltpu.VMEM((1024, 1024), BF16),
            pltpu.VMEM((4, 1024, 256), BF16),
            pltpu.VMEM((4, 1024, 256), BF16),
            pltpu.VMEM((8, 256, 256), BF16),
            pltpu.VMEM((4, 2, 256, 1024), BF16),
            pltpu.SemaphoreType.DMA((4, 2)),
        ],
        compiler_params=pltpu.CompilerParams(vmem_limit_bytes=66_000_000),
        cost_estimate=pl.CostEstimate(flops=7 * 10**9, bytes_accessed=12 * 2**20, transcendentals=0),
        name="panels",
    )(place, bucket_row, bucket_col, *arrays)


def moved(array, axis, by):
    count = lax.axis_size(axis)
    return lax.ppermute(array, axis, [(k, (k + by) % count) for k in range(count)])


def copies_for(array, axis):
    return jnp.broadcast_to(array, (lax.axis_size(axis), *array.shape))


def exchanged(copies, axis):
    return lax.all_to_all(copies, axis, split_axis=0, concat_axis=0, tiled=True)


def sent_to_all(array, axis):
    return exchanged(copies_for(array, axis), axis)


def per_device(diag_tile, left_row, right_row, right_col, bucket_row, bucket_col):
    zl, y, core = (lax.axis_index(axis) for axis in ROW)
    group = 2 * zl + y // 2
    wide = jnp.concatenate([diag_tile, diag_tile[:, :512]], axis=1)
    wide = jnp.concatenate([wide, diag_tile[:, 512:]], axis=1)
    part = lax.dynamic_slice_in_dim(wide, group * 128, SENT * 128, 1)
    near = jnp.stack([right_row, left_row]).transpose(0, 2, 1, 3)
    swapped = moved(near, "zh", 1)
    part = sent_to_all(part, ("zl", "zh"))
    part = sent_to_all(part, ("y", "x"))
    near = jnp.stack([near, swapped])
    other = moved(part, "c", 1)
    far = copies_for(right_col.transpose(1, 0, 2), ("zl", "y"))
    part, other, near, far = lax.optimization_barrier((part, other, near, far))
    far = exchanged(far, ("zl", "y"))
    near = [near, *[moved(near, "x", by) for by in range(1, 4)]]
    high, mid = chol_inverse(core[None], part, other)
    high, mid, far, *near = lax.optimization_barrier((high, mid, far, *near))
    far = (far, moved(far, "c", 1))
    place = jnp.stack([lax.axis_index(COL), lax.axis_index(ROW), lax.axis_index("x"), lax.axis_index("zh"), core])
    panel_row, panel_col, update_left = panels(place, bucket_row, bucket_col, high, mid, near, far)
    return panel_row.transpose(1, 0, 2), panel_col.transpose(1, 0, 2), update_left


def solution(mesh):
    fine = Mesh(mesh.devices.reshape(4, 4, 2, 4, 2), AXES)
    return jax.shard_map(
        per_device,
        mesh=fine,
        in_specs=(
            P(AXES, None),
            P(COL, ROW, None),
            P(COL, ROW, None),
            P(ROW, COL, None),
            P(ROW),
            P(COL),
        ),
        out_specs=(P(COL, ROW, None), P(ROW, COL, None), P(ROW, COL, None, None)),
        check_vma=False,
    )
```
